32 devices in a mesh: freq: 16 (over z, y, x), rhalf: 2 (over core).
Axes of the slice: x: 2, y: 2, z: 4, core: 2. Of those that a mesh axis runs over, the one named last changes fastest.
Arguments:
- reflection: bfloat16 [32, 2, 2048, 2048], P('freq', None, None, 'rhalf'), may hold values from -1 to 1, as said below
- focusing_direct: bfloat16 [2048, 2, 32, 128], P('rhalf', None, 'freq'), may hold values from -6 to 6
- arrival_index: int32 [2048, 128], P('rhalf'), may hold values from 8 to 23
Outputs:
- green: bfloat16 [128, 2048, 64], P('freq', 'rhalf')
The draws below stay inside these ranges and needn't reach their ends.
Inputs may be any that keep to these rules, and one draw needn't show every extreme that they name: For every frequency and part, reflection[k, c] is a symmetric 2048 x 2048 matrix (reciprocity).
All inputs are finite; a program needn't handle non-finite values.
Results may differ from the reference program's by a relative error of at most 0.017.
Values may be sent and summed in bfloat16 or wider, within the bound.
A program may use at most 64 MiB of HBM per device.

```python
import math
import jax
import jax.numpy as jnp
from jax import lax

NR = 2048
PTS = 128
NF = 32


def draw_reflection(key, part):

    def one_freq(index):
        subkey = jax.random.fold_in(key, index)
        base = jax.random.normal(subkey, (2, NR, NR), jnp.float32)
        symmetric = (base + jnp.swapaxes(base, 1, 2)) * (0.5 / NR ** 0.5)
        return jnp.clip(symmetric, -1.0, 1.0).astype(jnp.bfloat16)
    return lax.map(one_freq, jnp.arange(NF, dtype=jnp.int32))


def touch_ends(entries, rng, smallest, top_value):
    shape = entries.shape
    index_at = [jax.random.randint(jax.random.fold_in(rng, axis), (), 0, shape[axis]) for axis in range(len(shape))]
    entries = entries.at[tuple(index_at)].set(smallest)
    longest = shape.index(max(shape))
    index_at[longest] = (index_at[longest] + 1) % shape[longest]
    return entries.at[tuple(index_at)].set(top_value)


def block_scale(stream_key, dims, pieces, smallest, top_value):
    gain, own = 1.0, jax.random.fold_in(stream_key, 6)
    for dim, parts in pieces:
        draws = jnp.exp(jax.random.uniform(jax.random.fold_in(own, dim), (parts,), jnp.float32, smallest / len(pieces), top_value / len(pieces)))
        gain = gain * jnp.repeat(draws, dims[dim] // parts).reshape([-1 if axis == dim else 1 for axis in range(len(dims))])
    return gain


def noise(key, shape, width, bound, split=(), kind=jnp.bfloat16):
    level = block_scale(key, shape, split, -0.22, 0.18) if split else 1.0
    drawn = jax.random.normal(key, shape, jnp.float32) * width * level
    return jnp.minimum(jnp.maximum(drawn, -bound), bound).astype(kind)


def setup_inputs(seed: int = 0) -> dict:
    keys = jax.random.split(jax.random.key(seed), 4)
    reflection = draw_reflection(jax.random.fold_in(keys[3], 71), 0)
    focusing_direct = noise(keys[1], (NR, 2, NF, PTS), 1.0, 6.0, ((0, 2), (2, 16)))
    arrival_index = touch_ends(jax.random.randint(keys[2], (NR, PTS), 8, NF - 8), jax.random.fold_in(keys[2], 1), 8, (NF - 8) - 1).astype(jnp.int32)
    return {"reflection": reflection, "focusing_direct": focusing_direct, "arrival_index": arrival_index}


def transform_tables(nfreq):
    ntime = 2 * nfreq
    freqs = jnp.arange(nfreq, dtype=jnp.int32)
    times = jnp.arange(ntime, dtype=jnp.int32)
    phases = freqs[:, None] * times[None, :] % ntime
    angles = phases.astype(jnp.float32) * (2.0 * math.pi / ntime)
    norm_factor = 1.0 / math.sqrt(ntime)
    weights = jnp.where(freqs == 0, 1.0, 2.0).astype(jnp.float32)[:, None] * norm_factor
    inverse = jnp.stack([weights * jnp.cos(angles), -weights * jnp.sin(angles)])
    forward = jnp.stack([jnp.cos(angles).T, -jnp.sin(angles).T]) * norm_factor
    return (inverse, forward)

def pass_window(arrival, ntime):
    times = jnp.arange(ntime, dtype=jnp.int32)
    shifted = jnp.where(times < ntime // 2, times, times - ntime)
    return (jnp.abs(shifted)[None, :, None] < arrival[:, None, :]).astype(jnp.float32)

def apply_reflection(reflection, field, signed):

    def one_freq(pair):
        matrix, vectors = pair
        real_real = jnp.dot(matrix[0], vectors[:, 0], preferred_element_type=jnp.float32)
        imag_imag = jnp.dot(matrix[1], vectors[:, 1], preferred_element_type=jnp.float32)
        real_imag = jnp.dot(matrix[0], vectors[:, 1], preferred_element_type=jnp.float32)
        imag_real = jnp.dot(matrix[1], vectors[:, 0], preferred_element_type=jnp.float32)
        return jnp.stack([real_real - signed * imag_imag, real_imag + signed * imag_real])
    spectra = lax.map(one_freq, (reflection, jnp.transpose(field, (2, 0, 1, 3))))
    return jnp.transpose(spectra, (2, 1, 0, 3))

def to_time(spectra, inverse):
    return jnp.einsum('rcfp,cft->rtp', spectra, inverse, precision=lax.Precision.HIGHEST)

def to_freq(signal, forward):
    return jnp.einsum('rtp,ctf->rcfp', signal, forward, precision=lax.Precision.HIGHEST)

def reference(reflection, focusing_direct, arrival_index):
    nfreq = focusing_direct.shape[2]
    ntime = 2 * nfreq
    inverse, forward = transform_tables(nfreq)
    window = pass_window(arrival_index, ntime)
    first = apply_reflection(reflection, focusing_direct, 1.0)
    minus = to_freq(to_time(first, inverse) * window, forward).astype(jnp.bfloat16)
    second = apply_reflection(reflection, minus, -1.0)
    plus = (focusing_direct.astype(jnp.float32) + to_freq(to_time(second, inverse) * window, forward)).astype(jnp.bfloat16)
    third = apply_reflection(reflection, plus, 1.0)
    outside = 1.0 - jnp.transpose(window, (2, 0, 1))
    traces = jnp.einsum('rcfp,cft->prt', third, inverse, precision=lax.Precision.HIGHEST)
    return (traces * outside).astype(jnp.bfloat16)
```

```python
import math

import jax
import jax.numpy as jnp
from jax import lax
from jax.experimental import pallas as pl
from jax.experimental.pallas import tpu as pltpu
from jax.sharding import PartitionSpec as P

TILE = 512


def transform_tables(nfreq):
    ntime = 2 * nfreq
    freqs = jnp.arange(nfreq, dtype=jnp.int32)
    times = jnp.arange(ntime, dtype=jnp.int32)
    phases = freqs[:, None] * times[None, :] % ntime
    angles = phases.astype(jnp.float32) * (2.0 * math.pi / ntime)
    norm_factor = 1.0 / math.sqrt(ntime)
    weights = jnp.where(freqs == 0, 1.0, 2.0).astype(jnp.float32)[:, None] * norm_factor
    inverse = jnp.stack([weights * jnp.cos(angles), -weights * jnp.sin(angles)], axis=1)
    forward = jnp.stack([jnp.cos(angles), -jnp.sin(angles)], axis=1) * norm_factor
    return inverse.reshape(ntime, ntime), forward.reshape(ntime, ntime)


def signed_delay(ntime):
    times = jnp.arange(ntime, dtype=jnp.int32)
    return jnp.abs(jnp.where(times < ntime // 2, times, times - ntime))


def product_kernel(pieces, signed, r_ref, *refs):
    o_ref = refs[pieces]
    me = lax.axis_index("rhalf")
    freq = pl.program_id(0)
    by_real = by_imag = 0.0
    for j in range(pieces):
        x = refs[j][freq]
        rows, depth = x.shape
        owner = lax.rem(me + (pieces - j), pieces)
        at = pl.ds(pl.multiple_of(owner * depth, depth), depth)
        by_real += jnp.dot(x, r_ref[0, 0, at, :], preferred_element_type=jnp.float32)
        by_imag += jnp.dot(x, r_ref[0, 1, at, :], preferred_element_type=jnp.float32)
    half = rows // 2
    sums = (
        by_real[:half] - signed * by_imag[half:],
        by_real[half:] + signed * by_imag[:half],
    )
    if len(o_ref.shape) == 3:
        for c in range(2):
            o_ref[0, c * half : (c + 1) * half, :] = sums[c].astype(o_ref.dtype)
        return
    devices, _, _, here, tile = o_ref.shape
    for c in range(2):
        o_ref[:, 0, c] = sums[c].reshape(devices, here, tile).astype(o_ref.dtype)


def product(reflection, pieces, signed, devices):
    nf, _, full, own = reflection.shape
    _, rows, depth = pieces[0].shape
    here = rows // (2 * devices)
    tile = min(TILE, own)
    regroup = here % 8 == 0
    if regroup:
        out_shape = (devices, nf, 2, here, own)
        out_spec = pl.BlockSpec((devices, 1, 2, here, tile), lambda f, s: (0, f, 0, 0, s))
    else:
        out_shape = (nf, rows, own)
        out_spec = pl.BlockSpec((1, rows, tile), lambda f, s: (f, 0, s))
    spectra = pl.pallas_call(
        lambda *refs: product_kernel(len(pieces), signed, *refs),
        name="product_plus" if signed > 0 else "product_minus",
        out_shape=jax.ShapeDtypeStruct(out_shape, jnp.bfloat16),
        grid=(nf, own // tile),
        in_specs=[pl.BlockSpec((1, 2, full, tile), lambda f, s: (f, 0, 0, s))]
        + [pl.BlockSpec(memory_space=pltpu.VMEM) for _ in pieces],
        out_specs=out_spec,
        cost_estimate=pl.CostEstimate(
            flops=4 * nf * rows * full * own, bytes_accessed=4 * nf * full * own, transcendentals=0
        ),
    )(reflection, *pieces)
    if regroup:
        return spectra
    return jnp.transpose(spectra.reshape(nf, 2, devices, here, own), (2, 0, 1, 3, 4))


def exchange(blocks):
    return lax.all_to_all(blocks, "freq", split_axis=0, concat_axis=0, tiled=True)


def per_device(reflection, focusing_direct, arrival_index):
    own = focusing_direct.shape[0]
    freq_local = focusing_direct.shape[2]
    points = focusing_direct.shape[3]
    freq_devices = lax.axis_size("freq")
    halves = lax.axis_size("rhalf")
    nfreq = freq_local * freq_devices
    ntime = 2 * nfreq
    inverse, forward = transform_tables(nfreq)
    here = points // freq_devices
    my_index = lax.axis_index("freq")
    arrival = lax.dynamic_slice_in_dim(arrival_index, my_index * here, here, 1).T
    delay = signed_delay(ntime)
    inside = delay[:, None, None] < arrival[None]

    def reflect(field, signed):
        field = field.reshape(freq_local, 2 * points, own)
        pieces = [field]
        for shift in range(1, halves):
            pairs = [(i, (i + shift) % halves) for i in range(halves)]
            pieces.append(lax.ppermute(field, "rhalf", pairs))
        spectra = product(reflection, pieces, signed, freq_devices)
        return exchange(spectra).reshape(ntime, here, own)

    def mute(spectra):
        signal = jnp.einsum(
            "kps,kt->tps", spectra.astype(jnp.float32), inverse, precision=lax.Precision.HIGHEST
        )
        signal = jnp.where(inside, signal, 0.0)
        back = jnp.einsum("tps,kt->kps", signal, forward, precision=lax.Precision.HIGHEST)
        back = back.astype(jnp.bfloat16).reshape(freq_devices, freq_local, 2, here, own)
        back = jnp.transpose(exchange(back), (1, 2, 0, 3, 4))
        return back.reshape(freq_local, 2, points, own)

    direct = jnp.transpose(focusing_direct, (2, 1, 3, 0))
    minus = mute(reflect(direct, 1.0))
    change = mute(reflect(minus, -1.0))
    plus = (direct.astype(jnp.float32) + change.astype(jnp.float32)).astype(jnp.bfloat16)
    upgoing = reflect(plus, 1.0)
    traces = jnp.einsum(
        "kps,kt->pst", upgoing.astype(jnp.float32), inverse, precision=lax.Precision.HIGHEST
    )
    outside = delay >= arrival[:, :, None]
    return jnp.where(outside, traces, 0.0).astype(jnp.bfloat16)


def solution(mesh):
    return jax.shard_map(
        per_device,
        mesh=mesh,
        in_specs=(P("freq", None, None, "rhalf"), P("rhalf", None, "freq", None), P("rhalf", None)),
        out_specs=P("freq", "rhalf", None),
        check_vma=False,
    )
```
